16 devices in a mesh: rep: 1, r: 2 (over z), s: 8 (over x, y, core).
Axes of the slice: x: 2, y: 2, z: 2, core: 2. Of those that a mesh axis runs over, the one named last changes fastest.
Arguments:
- x: bfloat16 [16, 2048, 1536], P(('rep', 'r', 's'))
- dy: bfloat16 [16, 2048, 1536], P(('rep', 'r', 's'))
- w_gate: bfloat16 [2, 1536, 4224], P(None, 's')
- w_up: bfloat16 [2, 1536, 4224], P(None, 's')
- w_down: bfloat16 [2, 4224, 1536], P(None, 's')
Outputs:
- output 1: bfloat16 [16, 2048, 1536], P(('rep', 'r', 's'))
- output 2: bfloat16 [2, 1536, 4224], P('rep', 's')
- output 3: bfloat16 [2, 1536, 4224], P('rep', 's')
- output 4: bfloat16 [2, 4224, 1536], P('rep', 's')
All inputs are finite; a program needn't handle non-finite values.
Results may differ from the reference program's by a relative error of at most 0.018.
Values are sent between devices in bfloat16 or wider.
A program may use at most 2 GiB of HBM per device.

```python
import jax
import jax.numpy as jnp
from jax import lax

SEQUENCES = 16
TOKENS = 2048
D = 1536
FF = 4224
LAYERS = 2
NAMES = ("w_gate", "w_up", "w_down")
SHAPES = {"w_gate": (LAYERS, D, FF), "w_up": (LAYERS, D, FF), "w_down": (LAYERS, FF, D)}


def bump(key, n, height):
    away = (jnp.arange(n, dtype=jnp.int32) - jax.random.randint(key, (), 0, n, jnp.int32)) % n
    return jnp.where(away < n // 8, height, 1.0)


def together(key, own, strength):
    shared = jax.random.normal(key, own.shape[1:], jnp.float32)
    return (own + strength * shared) * lax.rsqrt(1 + strength * strength)


def setup_inputs(seed: int = 0, part: int = 0) -> dict:
    kx, kdy, ka, kb, kz, kf, kh, kl, *kw = jax.random.split(jax.random.key(seed), 8 + len(NAMES))
    kx, kdy, ka, kb = (jax.random.fold_in(k, part) for k in (kx, kdy, ka, kb))
    shape = (SEQUENCES, TOKENS, D)
    much_x, much_dy = jax.random.uniform(kz, (2,), jnp.float32, 0.0, 1.0)
    layers = 2.0 ** jax.random.uniform(kl, (LAYERS, 1, 1), jnp.float32, -1.0, 1.0)
    x = together(ka, jax.random.normal(kx, shape, jnp.float32), much_x) * bump(kf, D, 4.0)
    dy = together(kb, jax.random.normal(kdy, shape, jnp.float32), much_dy)
    drawn = {"x": x.astype(jnp.bfloat16), "dy": (dy * (SEQUENCES * TOKENS) ** -0.5).astype(jnp.bfloat16)}
    for key, name in zip(kw, NAMES, strict=True):
        w = jax.random.normal(key, SHAPES[name], jnp.float32) * SHAPES[name][1] ** -0.5
        drawn[name] = (w * {"w_gate": 1.0, "w_up": bump(kh, FF, 4.0), "w_down": layers}[name]).astype(jnp.bfloat16)
    return drawn


def matmul(a, w):
    return jnp.dot(a, w, preferred_element_type=jnp.float32).astype(jnp.bfloat16)


def normed(h):
    wide = h.astype(jnp.float32)
    scale = lax.rsqrt(jnp.mean(wide**2, -1, keepdims=True) + 1e-6)
    return (wide * scale).astype(jnp.bfloat16)


def layer(h, w):
    a = normed(h)
    gate = jnp.dot(a, w["w_gate"], preferred_element_type=jnp.float32)
    up = jnp.dot(a, w["w_up"], preferred_element_type=jnp.float32)
    return h + matmul((jax.nn.silu(gate) * up).astype(jnp.bfloat16), w["w_down"])


def stack(weights, h):
    return lax.scan(lambda h, w: (layer(h, w), None), h, weights)[0]


def reference(x, dy, w_gate, w_up, w_down):
    weights = dict(zip(NAMES, (w_gate, w_up, w_down), strict=True))

    def take(so_far, sequence):
        h, by_y = sequence
        _, back = jax.vjp(stack, weights, h)
        by_weights, by_h = back(by_y)
        return jax.tree.map(lambda total, term: total + term.astype(jnp.float32), so_far, by_weights), by_h

    none_yet = {name: jnp.zeros(w.shape, jnp.float32) for name, w in weights.items()}
    by_weights, by_x = lax.scan(take, none_yet, (x, dy))
    return (by_x, *(by_weights[name].astype(jnp.bfloat16) for name in NAMES))
```

```python
import functools

import jax
import jax.numpy as jnp
from jax import lax
from jax.experimental import pallas as pl
from jax.experimental.pallas import tpu as pltpu
from jax.sharding import PartitionSpec as P

NAMES = ("w_gate", "w_up", "w_down")
F32 = jnp.float32
BF16 = jnp.bfloat16
ANY = pl.BlockSpec(memory_space=pl.ANY)
MESH = pl.DeviceIdType.MESH
CHUNKS = 3
VMEM = 62 * 2**20


def dot(a, b, ca, cb):
    return lax.dot_general(a, b, (((ca,), (cb,)), ((), ())), preferred_element_type=F32)


class Gather:
    def __init__(self, w, n, out, send, recv, own, own_sem):
        s, z = lax.axis_index("s"), lax.axis_index("r")
        rep = lax.axis_index("rep")
        self.rows, width = w.shape[1], w.shape[2]
        self.step = self.rows // CHUNKS
        units = width // 128
        part = (units * 3 // 11) * 128
        region = width - part
        low = (region // 256) * 128
        start = pl.multiple_of(z * part, 128)
        mine = pl.multiple_of(z * region, 128)
        self.w, self.n, self.out, self.send, self.recv = w, n, out, send, recv
        self.own, self.own_sem = own, own_sem
        self.s = s
        self.cols = dict(region=(start, region), low=(start, low), high=(pl.multiple_of(start + low, 128), region - low), mine=(mine, part))
        self.x, self.y, self.core = (rep, z, s ^ 4), (rep, z, s ^ 2), (rep, z, s ^ 1)
        self.z = (rep, 1 - z, s)

    def at(self, who, i, cols):
        row = pl.multiple_of((self.s ^ who) * self.rows + i * self.step, 8)
        where = pl.ds(row, self.step)
        if cols is None:
            return self.out.at[where]
        return self.out.at[where, pl.ds(*self.cols[cols])]

    def copy(self, kind, i):
        k, to, who, cols = {
            "x": (0, self.x, 0, "region"),
            "y": (1, self.y, 0, "region"),
            "low": (2, self.y, 4, "low"),
            "high": (3, self.x, 2, "high"),
            "zx": (4, self.z, 4, "mine"),
            "zy": (5, self.z, 2, "mine"),
            "zd": (6, self.z, 6, "mine"),
            "c": (7, self.core, 0, None),
            "cx": (8, self.core, 4, None),
            "cy": (9, self.core, 2, None),
            "cd": (10, self.core, 6, None),
        }[kind]
        dst = self.at(who, i, cols)
        src = dst
        if who == 0:
            rows = pl.ds(i * self.step, self.step)
            src = self.w.at[self.n, rows] if cols is None else self.w.at[self.n, rows, pl.ds(*self.cols[cols])]
        j = k * CHUNKS + i
        return pltpu.make_async_remote_copy(
            src_ref=src, dst_ref=dst, send_sem=self.send.at[j], recv_sem=self.recv.at[j], device_id=to, device_id_type=MESH
        )

    def begin(self):
        barrier = pltpu.get_barrier_semaphore()
        for to in (self.x, self.y, self.z, self.core):
            pl.semaphore_signal(barrier, inc=1, device_id=to, device_id_type=MESH)
        pltpu.make_async_copy(self.w.at[self.n], self.own, self.own_sem.at[0]).start()
        pl.semaphore_wait(barrier, 4)
        for i in range(CHUNKS):
            self.copy("x", i).start()
            self.copy("y", i).start()
        for i in range(CHUNKS):
            self.copy("c", i).start()

    def keep(self):
        pltpu.make_async_copy(self.w.at[self.n], self.own, self.own_sem.at[0]).wait()
        self.kept().start()

    def kept(self):
        rows = pl.ds(pl.multiple_of(self.s * self.rows, 8), self.rows)
        return pltpu.make_async_copy(self.own, self.out.at[rows], self.own_sem.at[1])

    def first(self, i):
        for got, onward in (("x", ("low", "zx")), ("y", ("high", "zy"))):
            self.copy(got, i).wait_recv()
            for kind in onward:
                self.copy(kind, i).start()

    def second(self, i):
        self.copy("low", i).wait_recv()
        self.copy("high", i).wait_recv()
        self.copy("zd", i).start()

    def third(self, i):
        for got, onward in (("zx", "cx"), ("zy", "cy"), ("zd", "cd")):
            self.copy(got, i).wait_recv()
            self.copy(onward, i).start()

    def end(self):
        for i in range(CHUNKS):
            for kind in ("c", "cx", "cy", "cd"):
                self.copy(kind, i).wait_recv()
            for kind in ("x", "y", "low", "high", "zx", "zy", "zd", "c", "cx", "cy", "cd"):
                self.copy(kind, i).wait_send()
        self.kept().wait()


def columns(width):
    cuts = list(range(0, width - 1023, 1024))
    return [(c, (width if c == cuts[-1] else c + 1024)) for c in cuts]


def kernel(compute, n_in, n_out, steps, n, *refs):
    ins, w, outs, out = refs[:n_in], refs[n_in], refs[n_in + 1 : n_in + 1 + n_out], refs[n_in + 1 + n_out]
    own, own_sem, send, recv = refs[n_in + 2 + n_out :]
    gather = Gather(w, n, out, send, recv, own, own_sem)
    step = pl.program_id(0)

    @pl.when(step == 0)
    def _():
        gather.begin()

    if compute is not None:
        compute(*ins, *outs)
    events = [[gather.keep]]
    for i in range(CHUNKS + 2):
        for ahead, what in ((0, gather.first), (1, gather.second), (2, gather.third)):
            if 0 <= i - ahead < CHUNKS:
                events.append([functools.partial(what, i - ahead)])
    events.append([gather.end])
    for e, group in enumerate(events):
        @pl.when(step == min(e, steps - 1))
        def _(group=group):
            for event in group:
                event()


def with_gather(compute, ins, in_specs, outs, out_specs, steps, w, n, ident, flops):
    rows, width = w.shape[1], w.shape[2]
    body = functools.partial(kernel, compute, len(ins), len(outs), steps, n)
    return pl.pallas_call(
        body,
        grid=(steps,),
        in_specs=[*in_specs, ANY],
        out_specs=[*out_specs, ANY],
        out_shape=[*outs, jax.ShapeDtypeStruct((8 * rows, width), w.dtype)],
        scratch_shapes=[
            pltpu.VMEM((rows, width), w.dtype),
            pltpu.SemaphoreType.DMA((2,)),
            pltpu.SemaphoreType.DMA((11 * CHUNKS,)),
            pltpu.SemaphoreType.DMA((11 * CHUNKS,)),
        ],
        compiler_params=pltpu.CompilerParams(
            collective_id=ident, has_side_effects=True, vmem_limit_bytes=VMEM, dimension_semantics=("arbitrary",)
        ),
        cost_estimate=pl.CostEstimate(flops=flops, bytes_accessed=80 * 2**20, transcendentals=0),
        name=f"part_{ident}",
    )(*ins, w)


def gate_part(h, wg, gate, a):
    wide = h[...].astype(F32)
    a[...] = (wide * lax.rsqrt(jnp.mean(wide**2, -1, keepdims=True) + 1e-6)).astype(BF16)
    for lo, hi in columns(wg.shape[1]):
        gate[:, lo:hi] = dot(a[...], wg[:, lo:hi], 1, 0)


def up_part(a, wu, gate, up, act):
    for lo, hi in columns(wu.shape[1]):
        u = dot(a[...], wu[:, lo:hi], 1, 0)
        up[:, lo:hi] = u
        g = gate[:, lo:hi]
        act[:, lo:hi] = (g * jax.nn.sigmoid(g) * u).astype(BF16)


def down_part(act, wd, h, y):
    y[...] = h[...] + dot(act[...], wd[...], 1, 0).astype(BF16)


def solution(mesh):
    def flip(v, bit):
        return lax.ppermute(v, "s", [(i, i ^ bit) for i in range(8)])

    def across(v):
        other = lax.ppermute(v, "r", [(0, 1), (1, 0)])
        return (v.astype(F32) + other.astype(F32)).astype(BF16)

    def add(a, b):
        return (a.astype(F32) + b.astype(F32)).astype(BF16)

    def pick(v, i, axis):
        return lax.dynamic_index_in_dim(v, i, axis, keepdims=False)

    def queued(term):
        return across(lax.psum_scatter(term, "s", scatter_dimension=0, tiled=True))

    def cores(left, right):
        core = lax.axis_index("s") % 2
        tokens, rows = left.shape
        blocks = left.reshape(tokens, 4, 2, rows // 8)
        halves = [pick(blocks, i, 2).reshape(tokens, rows // 2) for i in (1 - core, core)]
        arrived = flip(dot(halves[0], right, 0, 0).astype(BF16), 1)
        both = (dot(halves[1], right, 0, 0) + arrived.astype(F32)).astype(BF16)
        return both.reshape(2, 2, rows // 8, -1)

    def sends(both):
        me = lax.axis_index("s")
        y, x = (me // 2) % 2, me // 4
        cut = (both.shape[-1] // 256) * 128
        return pick(both[..., :cut], 1 - x, 0), pick(both[..., cut:], 1 - y, 1)

    def scattered(both, out):
        me = lax.axis_index("s")
        y, x = (me // 2) % 2, me // 4
        cut = (both.shape[-1] // 256) * 128
        v = add(pick(both[..., :cut], x, 0), flip(out[0], 4))
        u = add(pick(both[..., cut:], y, 1), flip(out[1], 2))
        v = add(pick(v, y, 0), flip(pick(v, 1 - y, 0), 2))
        u = add(pick(u, x, 0), flip(pick(u, 1 - x, 0), 4))
        return jnp.concatenate([across(v), across(u)], axis=-1)

    def step(x, dy, w_gate, w_up, w_down):
        layers = w_gate.shape[0]
        tokens, d = x.shape[1:]
        ff = w_gate.shape[2]
        weights = (w_gate, w_up, w_down)
        steps = 8
        tile = tokens // steps
        flops = 2 * tokens * d * ff

        def rows(width):
            return pl.BlockSpec((tile, width), lambda i: (i, 0))

        def whole(height, width):
            return pl.BlockSpec((height, width), lambda i: (0, 0), pipeline_mode=pl.Buffered(1))

        def shape(width, dtype):
            return jax.ShapeDtypeStruct((tokens, width), dtype)

        h, kept = x[0], []
        (wg,) = with_gather(None, (), (), (), (), 1, w_gate, 0, 0, 1)
        for n in range(layers):
            gate, a, wu = with_gather(
                gate_part, (h, wg), (rows(d), whole(d, ff)), (shape(ff, F32), shape(d, BF16)), (rows(ff), rows(d)),
                steps, w_up, n, 3 * n + 1, flops,
            )
            up, act, wd = with_gather(
                up_part, (a, wu, gate), (rows(d), whole(d, ff), rows(ff)), (shape(ff, F32), shape(ff, BF16)), (rows(ff), rows(ff)),
                steps, w_down, n, 3 * n + 2, flops,
            )
            kept.append((h, a, wg, wu, wd, gate, up, act))
            if n + 1 < layers:
                h, wg = with_gather(
                    down_part, (act, wd, h), (rows(ff), whole(ff, d), rows(d)), (shape(d, BF16),), (rows(d),),
                    steps, w_gate, n + 1, 3 * n + 3, flops,
                )
        by_h, sums = dy[0], [None] * layers
        for n in reversed(range(layers)):
            h, a, wg, wu, wd, gate, up, act = kept[n]
            by_act = dot(by_h, wd, 1, 1).astype(BF16).astype(F32)
            sig = jax.nn.sigmoid(gate)
            by_up = (by_act * (gate * sig)).astype(BF16)
            by_gate = (by_act * up * (sig * (1 + gate * (1 - sig)))).astype(BF16)
            by_down = queued(dot(act, by_h, 0, 0).astype(BF16))
            if n:
                two = [queued(dot(a, v, 0, 0).astype(BF16)) for v in (by_gate, by_up)]
            else:
                two = []
                for v in (by_gate, by_up):
                    both = cores(a, v)
                    out = sends(both)
                    out, by_gate, by_up = lax.optimization_barrier((out, by_gate, by_up))
                    two.append(scattered(both, out))
            by_a = (dot(by_gate, wg, 1, 1) + dot(by_up, wu, 1, 1)).astype(BF16).astype(F32)
            wide = h.astype(F32)
            scale = lax.rsqrt(jnp.mean(wide**2, -1, keepdims=True) + 1e-6)
            along = jnp.mean(by_a * wide, -1, keepdims=True)
            by_h = by_h + (scale * (by_a - wide * (scale * scale * along))).astype(BF16)
            sums[n] = (*two, by_down)
        return (by_h[None], *(jnp.stack([sums[n][i] for n in range(layers)]) for i in range(3)))

    states, cut = P(("rep", "r", "s"), None, None), P(None, "s", None)
    return jax.shard_map(
        step,
        mesh=mesh,
        in_specs=(states, states) + (cut,) * 3,
        out_specs=(states,) + (P("rep", "s", None),) * 3,
        check_vma=False,
    )
```

```python
import functools

import jax
import jax.numpy as jnp
from jax import lax
from jax.experimental import pallas as pl
from jax.experimental.pallas import tpu as pltpu
from jax.sharding import PartitionSpec as P

F32 = jnp.float32
BF16 = jnp.bfloat16
ANY = pl.BlockSpec(memory_space=pl.ANY)
MESH = pl.DeviceIdType.MESH
CHUNKS = 6
AHEAD = 2
VMEM = 62 * 2**20


def dot(a, b, ca, cb):
    return lax.dot_general(a, b, (((ca,), (cb,)), ((), ())), preferred_element_type=F32)


class Gather:
    def __init__(self, weights, numbers, outs, owns, own_sem, send, recv):
        s, z, rep = lax.axis_index("s"), lax.axis_index("r"), lax.axis_index("rep")
        self.weights, self.numbers, self.outs, self.owns = weights, numbers, outs, owns
        self.send, self.recv, self.own_sem = send, recv, own_sem
        self.s, self.group = s, z
        self.pieces = CHUNKS * len(weights)
        self.x, self.y, self.core = (rep, z, s ^ 4), (rep, z, s ^ 2), (rep, z, s ^ 1)
        self.z = (rep, 1 - z, s)

    def cols(self, w, what):
        units = w.shape[2] // 128
        part = ((units + 1) // 3) * 128
        region = w.shape[2] - part
        low = (region // 256) * 128
        start = self.group * part
        return {
            "region": pl.ds(pl.multiple_of(start, 128), region),
            "low": pl.ds(pl.multiple_of(start, 128), low),
            "high": pl.ds(pl.multiple_of(start + low, 128), region - low),
            "mine": pl.ds(pl.multiple_of(self.group * region, 128), part),
        }[what]

    def copy(self, kind, i):
        k, to, who, cols = {
            "x": (0, self.x, 0, "region"),
            "y": (1, self.y, 0, "region"),
            "low": (2, self.y, 4, "low"),
            "high": (3, self.x, 2, "high"),
            "zx": (4, self.z, 4, "mine"),
            "zy": (5, self.z, 2, "mine"),
            "zd": (6, self.z, 6, "mine"),
            "c": (7, self.core, 0, None),
            "cx": (8, self.core, 4, None),
            "cy": (9, self.core, 2, None),
            "cd": (10, self.core, 6, None),
        }[kind]
        which, i_in = divmod(i, CHUNKS)
        w, n, out = self.weights[which], self.numbers[which], self.outs[which]
        rows = w.shape[1]
        height = rows // CHUNKS
        at = (pl.ds(pl.multiple_of((self.s ^ who) * rows + i_in * height, 8), height),)
        own = (n, pl.ds(i_in * height, height))
        if cols is not None:
            at, own = (*at, self.cols(w, cols)), (*own, self.cols(w, cols))
        dst = out.at[at]
        src = dst if who else w.at[own]
        j = k * self.pieces + i
        return pltpu.make_async_remote_copy(
            src_ref=src, dst_ref=dst, send_sem=self.send.at[j], recv_sem=self.recv.at[j], device_id=to, device_id_type=MESH
        )

    def held(self, which):
        w, n, out, own = self.weights[which], self.numbers[which], self.outs[which], self.owns[which]
        rows = pl.ds(pl.multiple_of(self.s * w.shape[1], 8), w.shape[1])
        return (
            pltpu.make_async_copy(w.at[n], own, self.own_sem.at[2 * which]),
            pltpu.make_async_copy(own, out.at[rows], self.own_sem.at[2 * which + 1]),
        )

    def begin(self):
        barrier = pltpu.get_barrier_semaphore()
        for to in (self.x, self.y, self.z, self.core):
            pl.semaphore_signal(barrier, inc=1, device_id=to, device_id_type=MESH)
        for which in range(len(self.weights)):
            self.held(which)[0].start()
        pl.semaphore_wait(barrier, 4)
        for i in range(AHEAD):
            self.issue(i)

    def issue(self, i):
        for kind in ("x", "y", "c"):
            self.copy(kind, i).start()

    def keep(self):
        for which in range(len(self.weights)):
            self.held(which)[0].wait()
            self.held(which)[1].start()

    def first(self, i):
        if i + AHEAD < self.pieces:
            self.issue(i + AHEAD)
        for got, onward in (("x", ("low", "zx")), ("y", ("high", "zy"))):
            self.copy(got, i).wait_recv()
            for kind in onward:
                self.copy(kind, i).start()

    def second(self, i):
        self.copy("low", i).wait_recv()
        self.copy("high", i).wait_recv()
        self.copy("zd", i).start()

    def third(self, i):
        for got, onward in (("zx", "cx"), ("zy", "cy"), ("zd", "cd")):
            self.copy(got, i).wait_recv()
            self.copy(onward, i).start()

    def end(self):
        for i in range(self.pieces):
            for kind in ("c", "cx", "cy", "cd"):
                self.copy(kind, i).wait_recv()
            for kind in ("x", "y", "low", "high", "zx", "zy", "zd", "c", "cx", "cy", "cd"):
                self.copy(kind, i).wait_send()
        for which in range(len(self.weights)):
            self.held(which)[1].wait()

    def events(self):
        found = [self.keep]
        for i in range(self.pieces + 2):
            for ahead, what in ((0, self.first), (1, self.second), (2, self.third)):
                if 0 <= i - ahead < self.pieces:
                    found.append(functools.partial(what, i - ahead))
        return [*found, self.end]


def columns(width):
    cuts = list(range(0, width - 1023, 1024))
    return [(c, (width if c == cuts[-1] else c + 1024)) for c in cuts]


def kernel(compute, n_in, n_out, steps, numbers, *refs):
    k = len(numbers)
    cuts = [n_in, k, n_out, k, k]
    groups = []
    for size in cuts:
        groups.append(refs[:size])
        refs = refs[size:]
    ins, weights, outs, wholes, owns = groups
    gather = Gather(weights, numbers, wholes, owns, *refs)
    step = pl.program_id(0)

    @pl.when(step == 0)
    def _():
        gather.begin()

    if compute is not None:
        compute(*ins, *outs)
    events = gather.events()
    for t in range(steps):
        due = events[t * len(events) // steps : (t + 1) * len(events) // steps]

        @pl.when(step == t)
        def _(due=due):
            for event in due:
                event()


def with_gather(compute, ins, in_specs, outs, out_specs, steps, weights, ident, flops):
    arrays = [w for w, _ in weights]
    body = functools.partial(kernel, compute, len(ins), len(outs), steps, [n for _, n in weights])
    copies = 11 * CHUNKS * len(weights)
    return pl.pallas_call(
        body,
        grid=(steps,),
        in_specs=[*in_specs, *(ANY for _ in arrays)],
        out_specs=[*out_specs, *(ANY for _ in arrays)],
        out_shape=[*outs, *(jax.ShapeDtypeStruct((8 * w.shape[1], w.shape[2]), w.dtype) for w in arrays)],
        scratch_shapes=[
            *(pltpu.VMEM(w.shape[1:], w.dtype) for w in arrays),
            pltpu.SemaphoreType.DMA((2 * len(arrays),)),
            pltpu.SemaphoreType.DMA((copies,)),
            pltpu.SemaphoreType.DMA((copies,)),
        ],
        compiler_params=pltpu.CompilerParams(
            collective_id=ident, has_side_effects=True, vmem_limit_bytes=VMEM, dimension_semantics=("arbitrary",)
        ),
        cost_estimate=pl.CostEstimate(flops=flops, bytes_accessed=80 * 2**20, transcendentals=0),
    )(*ins, *arrays)


def both_part(h, wg, wu, gate, up, act, a):
    wide = h[...].astype(F32)
    a[...] = (wide * lax.rsqrt(jnp.mean(wide**2, -1, keepdims=True) + 1e-6)).astype(BF16)
    for lo, hi in columns(wg.shape[1]):
        g = dot(a[...], wg[:, lo:hi], 1, 0)
        u = dot(a[...], wu[:, lo:hi], 1, 0)
        gate[:, lo:hi] = g
        up[:, lo:hi] = u
        act[:, lo:hi] = (g * jax.nn.sigmoid(g) * u).astype(BF16)


def down_part(act, wd, h, y):
    y[...] = h[...] + dot(act[...], wd[...], 1, 0).astype(BF16)


def back_part(by_h, wd, gate, up, by_gate, by_up):
    for lo, hi in columns(wd.shape[0]):
        by_act = dot(by_h[...], wd[lo:hi, :], 1, 1).astype(BF16).astype(F32)
        g = gate[:, lo:hi]
        sig = jax.nn.sigmoid(g)
        by_up[:, lo:hi] = (by_act * (g * sig)).astype(BF16)
        by_gate[:, lo:hi] = (by_act * up[:, lo:hi] * (sig * (1 + g * (1 - sig)))).astype(BF16)


def into_part(by_gate, by_up, wg, wu, h, by_h, *rest):
    by_a = dot(by_gate[...], wg[...], 1, 1) + dot(by_up[...], wu[...], 1, 1)
    by_a = by_a.astype(BF16).astype(F32)
    wide = h[...].astype(F32)
    scale = lax.rsqrt(jnp.mean(wide**2, -1, keepdims=True) + 1e-6)
    along = jnp.mean(by_a * wide, -1, keepdims=True)
    rest[-1][...] = by_h[...] + (scale * (by_a - wide * (scale * scale * along))).astype(BF16)


def alone(body, ins, in_specs, outs, out_specs, steps, flops, aliases=None):
    return pl.pallas_call(
        body,
        grid=(steps,),
        in_specs=list(in_specs),
        out_specs=list(out_specs),
        out_shape=list(outs),
        input_output_aliases=aliases or {},
        compiler_params=pltpu.CompilerParams(vmem_limit_bytes=VMEM, dimension_semantics=("arbitrary",)),
        cost_estimate=pl.CostEstimate(flops=flops, bytes_accessed=80 * 2**20, transcendentals=0),
    )(*ins)


def solution(mesh):
    def flip(v, bit):
        return lax.ppermute(v, "s", [(i, i ^ bit) for i in range(8)])

    def across(v):
        other = lax.ppermute(v, "r", [(0, 1), (1, 0)])
        return (v.astype(F32) + other.astype(F32)).astype(BF16)

    def add(a, b):
        return (a.astype(F32) + b.astype(F32)).astype(BF16)

    def pick(v, i, axis):
        return lax.dynamic_index_in_dim(v, i, axis, keepdims=False)

    def queued(term):
        return lax.psum_scatter(term, "s", scatter_dimension=0, tiled=True)

    def place():
        me = lax.axis_index("s")
        return me % 2, (me // 2) % 2, me // 4

    def cut(v):
        at = (v.shape[-1] // 256) * 128
        return v[..., :at], v[..., at:]

    def sends(v):
        _, y, x = place()
        left, right = cut(v)
        return pick(left, 1 - x, 0), pick(right, 1 - y, 1)

    def stage(v, out):
        _, y, x = place()
        left, right = cut(v)
        got_left = flip(out[0], 4)
        got_right = flip(out[1], 2)
        left, right = add(pick(left, x, 0), got_left), add(pick(right, y, 1), got_right)
        return (left, right), (pick(left, 1 - y, 0), pick(right, 1 - x, 0))

    def last(kept, out):
        _, y, x = place()
        got_left = flip(out[0], 2)
        got_right = flip(out[1], 4)
        return jnp.concatenate([add(pick(kept[0], y, 0), got_left), add(pick(kept[1], x, 0), got_right)], axis=-1)

    tie = lax.optimization_barrier

    def step(x, dy, w_gate, w_up, w_down):
        layers = w_gate.shape[0]
        tokens, d = x.shape[1:]
        ff = w_gate.shape[2]
        flops = 2 * tokens * d * ff

        def rows(width, steps):
            return pl.BlockSpec((tokens // steps, width), lambda i: (i, 0))

        def whole(height, width):
            return pl.BlockSpec((height, width), lambda i: (0, 0), pipeline_mode=pl.Buffered(1))

        def shape(width, dtype):
            return jax.ShapeDtypeStruct((tokens, width), dtype)

        h, kept = x[0], []
        wg, wu = with_gather(None, (), (), (), (), 1, ((w_gate, 0), (w_up, 0)), 0, 1)
        for n in range(layers):
            more = n + 1 < layers
            gate, up, act, a, wd, *ahead = with_gather(
                both_part,
                (h, wg, wu),
                (rows(d, 16), whole(d, ff), whole(d, ff)),
                (shape(ff, F32), shape(ff, F32), shape(ff, BF16), shape(d, BF16)),
                (rows(ff, 16), rows(ff, 16), rows(ff, 16), rows(d, 16)),
                16,
                ((w_down, n), (w_gate, n + 1)) if more else ((w_down, n),),
                2 * n + 1,
                2 * flops,
            )
            kept.append((h, a, wg, wu, wd, gate, up, act))
            if more:
                wg = ahead[0]
                h, wu = with_gather(
                    down_part, (act, wd, h), (rows(ff, 16), whole(ff, d), rows(d, 16)), (shape(d, BF16),), (rows(d, 16),),
                    16, ((w_up, n + 1),), 2 * n + 2, flops,
                )
        by_h, sums = dy[0], [None] * layers
        core, _, _ = place()
        for n in reversed(range(layers)):
            h, a, wg, wu, wd, gate, up, act = kept[n]
            term = dot(act, by_h, 0, 0).astype(BF16)
            term, by_h = tie((term, by_h))
            by_down = queued(term)
            by_gate, by_up = alone(
                back_part,
                (by_h, wd, gate, up),
                (rows(d, 8), whole(ff, d), rows(ff, 8), rows(ff, 8)),
                (shape(ff, BF16),) * 2,
                (rows(ff, 8),) * 2,
                8,
                flops,
            )
            if n:
                term, a = tie((dot(a, by_gate, 0, 0).astype(BF16), a))
                by_wg = queued(term)
                term, by_gate, by_up = tie((dot(a, by_up, 0, 0).astype(BF16), by_gate, by_up))
                by_wu = queued(term)
            else:
                blocks = a.reshape(tokens, 4, 2, d // 8)
                theirs, ours = (pick(blocks, i, 2).reshape(tokens, d // 2) for i in (1 - core, core))
                theirs, by_up = tie((theirs, by_up))
                go, ours = tie((dot(theirs, by_up, 0, 0).astype(BF16), ours))
                got = flip(go, 1)
                rise = dot(ours, by_up, 0, 0)
                rise, got = tie((rise, got))
                rise = (rise + got.astype(F32)).astype(BF16).reshape(2, 2, d // 8, ff)
                out, by_gate = tie((sends(rise), by_gate))
                term = dot(a, by_gate, 0, 0).astype(BF16)
                term, by_gate = tie((term, by_gate))
                by_wg = queued(term)
                rise, out = stage(rise, out)
                out, by_up = tie((out, by_up))

            def into(part, steps, ins):
                def block(width):
                    return pl.BlockSpec((256, width), lambda i: (part * steps + i, 0))

                return alone(
                    into_part,
                    ins,
                    (block(ff), block(ff), whole(d, ff), whole(d, ff), block(d), block(d), *(ANY for _ in ins[6:])),
                    (shape(d, BF16),),
                    (block(d),),
                    steps,
                    2 * flops * steps * 256 // tokens,
                    {6: 0} if ins[6:] else None,
                )[0]

            if n:
                by_h = into(0, tokens // 256, (by_gate, by_up, wg, wu, h, by_h))
            else:
                some = into(0, tokens // 512, (by_gate, by_up, wg, wu, h, by_h))
                by_wu = last(rise, out)
                some, by_wu = tie((some, by_wu))
                by_h = into(1, tokens // 512, (by_gate, by_up, wg, wu, h, by_h, some))
            by_wg, by_wu, by_down = across(by_wg), across(by_wu), across(by_down)
            sums[n] = [by_wg, by_wu, by_down]
        return (by_h[None], *(jnp.stack([sums[n][i] for n in range(layers)]) for i in range(3)))

    states, split = P(("rep", "r", "s"), None, None), P(None, "s", None)
    return jax.shard_map(
        step,
        mesh=mesh,
        in_specs=(states, states) + (split,) * 3,
        out_specs=(states,) + (P("rep", "s", None),) * 3,
        check_vma=False,
    )
```
